8 devices in a mesh: stage: 4 (over z, y, x), data: 2 (over core).
Axes of the slice: x: 2, y: 2, z: 1, core: 2. Of those that a mesh axis runs over, the one named last changes fastest.
Arguments:
- x_in: bfloat16 [4, 8192, 1024], P(None, 'data')
- targets: bfloat16 [4, 8192, 1024], P(None, 'data')
- w_work: bfloat16 [4, 1, 8388608], P('stage')
- w_master: float32 [4, 1, 8388608], P('stage', None, 'data')
- m_prior: float32 [4, 1, 8388608], P('stage', None, 'data')
- v_prior: float32 [4, 1, 8388608], P('stage', None, 'data')
- clip_tau: float32 [], replicated
Outputs:
- output 1: float32 [], replicated
- output 2: bfloat16 [4, 1, 8388608], P('stage')
- output 3: float32 [4, 1, 8388608], P('stage', None, 'data')
- output 4: float32 [4, 1, 8388608], P('stage', None, 'data')
- output 5: float32 [4, 1, 8388608], P('stage', None, 'data')
All inputs are finite; a program needn't handle non-finite values.
Results may differ from the reference program's by a relative error of at most 0.001.
Values are sent between devices in bfloat16 or wider.
A program may use at most 1 GiB of HBM per device.

```python
import math
import jax
import jax.numpy as jnp
from jax import lax

D_MODEL = 1024
LAYERS = 1
MICROBATCHES = 4
TOK_DEV = 4096
STAGES = 4
DATA_SIZE = 2
ADAM_STEP = 10

ROW_COUNT = DATA_SIZE * TOK_DEV
HALF_LEN = 4 * D_MODEL * D_MODEL
FLAT_LEN = 2 * HALF_LEN
ADAM_BETA1 = 0.9
ADAM_BETA2 = 0.95
ADAM_EPS = 1e-8
WEIGHT_DECAY = 0.1
LEARN_RATE = 0.05 / math.sqrt(D_MODEL)


def gelu_tanh(z_val):
    return jax.nn.gelu(z_val, approximate=True)


def split_layer(w_flat):
    return w_flat[:HALF_LEN].reshape(D_MODEL, 4 * D_MODEL), w_flat[HALF_LEN:].reshape(4 * D_MODEL, D_MODEL)


def layer_forward(hidden, w_flat):
    w_in, w_out = split_layer(w_flat)
    pre_act = jnp.dot(hidden, w_in, preferred_element_type=jnp.float32).astype(jnp.bfloat16)
    act_bf = gelu_tanh(pre_act.astype(jnp.float32)).astype(jnp.bfloat16)
    out_rows = (hidden.astype(jnp.float32) + jnp.dot(act_bf, w_out, preferred_element_type=jnp.float32)).astype(jnp.bfloat16)
    return out_rows, pre_act


def layer_backward(hidden, pre_act, grad_h, w_flat):
    w_in, w_out = split_layer(w_flat)
    act_f, gelu_pull = jax.vjp(gelu_tanh, pre_act.astype(jnp.float32))
    act_bf = act_f.astype(jnp.bfloat16)
    grad_act = jnp.dot(grad_h, w_out.T, preferred_element_type=jnp.float32)
    grad_pre = gelu_pull(grad_act)[0].astype(jnp.bfloat16)
    grad_in = (grad_h.astype(jnp.float32) + jnp.dot(grad_pre, w_in.T, preferred_element_type=jnp.float32)).astype(jnp.bfloat16)
    g_first = jnp.dot(hidden.T, grad_pre, preferred_element_type=jnp.float32)
    g_second = jnp.dot(act_bf.T, grad_h, preferred_element_type=jnp.float32)
    return grad_in, jnp.concatenate([g_first.reshape(-1), g_second.reshape(-1)])


def loss_and_grads(x_in, targets, w_work):
    w_layers = w_work.reshape(-1, w_work.shape[-1])
    token_count = x_in.shape[0] * x_in.shape[1]

    def fwd_body(hidden, w_flat):
        out_rows, pre_act = layer_forward(hidden, w_flat)
        return out_rows, (hidden, pre_act)

    def bwd_body(grad_h, layer_data):
        hidden, pre_act, w_flat = layer_data
        return layer_backward(hidden, pre_act, grad_h, w_flat)

    def micro_step(scan_state, micro_batch):
        grad_acc, loss_acc = scan_state
        x_rows, t_rows = micro_batch
        y_rows, saved_acts = lax.scan(fwd_body, x_rows, w_layers)
        residual = y_rows.astype(jnp.float32) - t_rows.astype(jnp.float32)
        loss_acc = loss_acc + 0.5 * jnp.sum(residual * residual)
        grad_top = (residual / token_count).astype(jnp.bfloat16)
        _, layer_grads = lax.scan(bwd_body, grad_top, (saved_acts[0], saved_acts[1], w_layers), reverse=True)
        return (grad_acc + layer_grads, loss_acc), None

    start_state = (jnp.zeros(w_layers.shape, jnp.float32), jnp.zeros((), jnp.float32))
    (grad_acc, loss_acc), _ = lax.scan(micro_step, start_state, (x_in, targets))
    return loss_acc / token_count, grad_acc.reshape(w_work.shape)


def setup_inputs(seed: int = 0) -> dict:
    root_key = jax.random.key(seed)
    sub_keys = jax.random.split(root_key, 7)
    depth_n = STAGES * LAYERS
    x_in = jax.random.normal(sub_keys[0], (MICROBATCHES, ROW_COUNT, D_MODEL), jnp.float32).astype(jnp.bfloat16)
    targets = jax.random.normal(sub_keys[1], (MICROBATCHES, ROW_COUNT, D_MODEL), jnp.float32).astype(jnp.bfloat16)
    w_first = jax.random.normal(sub_keys[2], (STAGES, LAYERS, HALF_LEN), jnp.float32) / math.sqrt(D_MODEL)
    w_second = jax.random.normal(sub_keys[3], (STAGES, LAYERS, HALF_LEN), jnp.float32) / math.sqrt(4 * D_MODEL * depth_n)
    w_master = jnp.concatenate([w_first, w_second], axis=-1)
    w_work = w_master.astype(jnp.bfloat16)
    _, grads = loss_and_grads(x_in, targets, w_work)
    grad_norm = jnp.sqrt(jnp.sum(grads * grads))
    first_part = grads[:, :, :HALF_LEN]
    second_part = grads[:, :, HALF_LEN:]
    first_rms = jnp.sqrt(jnp.mean(first_part * first_part, axis=-1, keepdims=True))
    second_rms = jnp.sqrt(jnp.mean(second_part * second_part, axis=-1, keepdims=True))
    grad_scale = 0.4 * jnp.where(jnp.arange(FLAT_LEN) < HALF_LEN, first_rms, second_rms)
    m_prior = (1.0 - ADAM_BETA1) * grad_scale * jax.random.normal(sub_keys[4], w_master.shape, jnp.float32)
    v_prior = (1.0 - ADAM_BETA2) * grad_scale * grad_scale * jax.random.uniform(sub_keys[5], w_master.shape, jnp.float32, 0.5, 2.0)
    clip_tau = grad_norm * jax.random.uniform(sub_keys[6], (), jnp.float32, 0.3, 0.5)
    return {'x_in': x_in, 'targets': targets, 'w_work': w_work, 'w_master': w_master, 'm_prior': m_prior, 'v_prior': v_prior, 'clip_tau': clip_tau}


def reference(x_in, targets, w_work, w_master, m_prior, v_prior, clip_tau):
    loss_mean, grads = loss_and_grads(x_in, targets, w_work)
    grad_norm = jnp.sqrt(jnp.sum(grads * grads))
    clip_scale = jnp.minimum(1.0, clip_tau / grad_norm)
    scaled = clip_scale * grads
    m_new = ADAM_BETA1 * m_prior + (1.0 - ADAM_BETA1) * scaled
    v_new = ADAM_BETA2 * v_prior + (1.0 - ADAM_BETA2) * scaled * scaled
    m_hat = m_new / (1.0 - ADAM_BETA1 ** ADAM_STEP)
    v_hat = v_new / (1.0 - ADAM_BETA2 ** ADAM_STEP)
    w_new = w_master - LEARN_RATE * (m_hat / (jnp.sqrt(v_hat) + ADAM_EPS) + WEIGHT_DECAY * w_master)
    return (loss_mean, w_new.astype(jnp.bfloat16), w_new, m_new, v_new)
```

```python
import functools
import math
import jax
import jax.numpy as jnp
from jax import lax
from jax.experimental import pallas as pl
from jax.experimental.pallas import tpu as pltpu
from jax.sharding import PartitionSpec as P

B1 = 0.9
B2 = 0.95
EPS = 1e-8
DECAY = 0.1
STEP = 10
LR_BASE = 0.05
F32 = jnp.float32
BF16 = jnp.bfloat16
K0 = math.sqrt(2.0 / math.pi)
K1 = 0.044715


def to_tiles(w):
    r, c = w.shape
    return w.reshape(r // 8, 8, c // 128, 128).transpose(0, 2, 1, 3).reshape(r * c // 1024, 8, 128)


def from_tiles(t, r, c):
    return t.reshape(r // 8, c // 128, 8, 128).transpose(0, 2, 1, 3).reshape(r, c)


def dot(a, b, dims):
    return lax.dot_general(a, b, (dims, ((), ())), preferred_element_type=F32)


def params(n):
    return pltpu.CompilerParams(dimension_semantics=('arbitrary',) * n, vmem_limit_bytes=56 * 2**20)


def cost(rows, d, f):
    return pl.CostEstimate(flops=2 * rows * d * f, bytes_accessed=80 * 2**20, transcendentals=rows * f)


def up_kernel(x_ref, w_ref, u_ref, a_ref):
    for i in range(w_ref.shape[1] // 256):
        s = (slice(None), pl.ds(i * 256, 256))
        u = dot(x_ref[...], w_ref[s], ((1,), (0,))).astype(BF16)
        u_ref[s] = u
        z = u.astype(F32)
        a_ref[s] = (z * jax.nn.sigmoid(z * (2.0 * K0 + (2.0 * K0 * K1) * (z * z)))).astype(BF16)


def up(x, stack, base):
    rows, d = x.shape
    f = 4 * d
    bm = 1024
    return pl.pallas_call(
        up_kernel,
        grid=(f // d, rows // bm),
        in_specs=[pl.BlockSpec((bm, d), lambda j, i: (i, 0)), pl.BlockSpec((d, d), lambda j, i: (base * 4 + j, 0))],
        out_specs=[pl.BlockSpec((bm, d), lambda j, i: (i, j))] * 2,
        out_shape=[jax.ShapeDtypeStruct((rows, f), BF16)] * 2,
        compiler_params=params(2), cost_estimate=cost(rows, d, f), name='up',
    )(x, stack)


def down_kernel(a_ref, w_ref, h_ref, o_ref):
    for i in range(o_ref.shape[1] // 512):
        s = (slice(None), pl.ds(i * 512, 512))
        o_ref[s] = (h_ref[s].astype(F32) + dot(a_ref[...], w_ref[s], ((1,), (0,)))).astype(BF16)


def down(a, stack, base, h):
    rows, f = a.shape
    d = h.shape[1]
    bm = 512
    return pl.pallas_call(
        down_kernel,
        grid=(rows // bm,),
        in_specs=[pl.BlockSpec((bm, f), lambda i: (i, 0)), pl.BlockSpec((f, d), lambda i: (base, 0)),
                  pl.BlockSpec((bm, d), lambda i: (i, 0))],
        out_specs=pl.BlockSpec((bm, d), lambda i: (i, 0)),
        out_shape=jax.ShapeDtypeStruct((rows, d), BF16),
        compiler_params=params(1), cost_estimate=cost(rows, d, f), name='down',
    )(a, stack, h)


def du_kernel(g_ref, w_ref, u_ref, o_ref):
    for i in range(g_ref.shape[0] // 256):
        s = pl.ds(i * 256, 256)
        e = dot(g_ref[s, :], w_ref[...], ((1,), (1,)))
        z = u_ref[s, :].astype(F32)
        zz = z * z
        p = jax.nn.sigmoid(z * (2.0 * K0 + (2.0 * K0 * K1) * zz))
        o_ref[s, :] = (e * (p + (p - p * p) * (z * (2.0 * K0 + (6.0 * K0 * K1) * zz)))).astype(BF16)


def du_of(g, stack, base, u):
    rows, d = g.shape
    f = 4 * d
    bm = 1024
    return pl.pallas_call(
        du_kernel,
        grid=(f // d, rows // bm),
        in_specs=[pl.BlockSpec((bm, d), lambda j, i: (i, 0)), pl.BlockSpec((d, d), lambda j, i: (base * 4 + j, 0)),
                  pl.BlockSpec((bm, d), lambda j, i: (i, j))],
        out_specs=pl.BlockSpec((bm, d), lambda j, i: (i, j)),
        out_shape=jax.ShapeDtypeStruct((rows, f), BF16),
        compiler_params=params(2), cost_estimate=cost(rows, d, f), name='du',
    )(g, stack, u)


def dx_kernel(u_ref, w_ref, g_ref, o_ref):
    d = o_ref.shape[1]
    acc = g_ref[...].astype(F32)
    for q in range(w_ref.shape[0] // d):
        acc = acc + dot(u_ref[:, q * d:(q + 1) * d], w_ref[pl.ds(q * d, d), :], ((1,), (1,)))
    o_ref[...] = acc.astype(BF16)


def dx(du, stack, base, g):
    rows, f = du.shape
    d = g.shape[1]
    bm = 512
    return pl.pallas_call(
        dx_kernel,
        grid=(rows // bm,),
        in_specs=[pl.BlockSpec((bm, f), lambda i: (i, 0)), pl.BlockSpec((f, d), lambda i: (base, 0)),
                  pl.BlockSpec((bm, d), lambda i: (i, 0))],
        out_specs=pl.BlockSpec((bm, d), lambda i: (i, 0)),
        out_shape=jax.ShapeDtypeStruct((rows, d), BF16),
        compiler_params=params(1), cost_estimate=cost(rows, d, f), name='dx',
    )(du, stack, g)


def adam_kernel(lr, c_ref, g_ref, w_ref, m_ref, v_ref, wo_ref, mo_ref, vo_ref, wb_ref):
    sg = c_ref[0] * g_ref[...]
    m = B1 * m_ref[...] + (1.0 - B1) * sg
    v = B2 * v_ref[...] + (1.0 - B2) * sg * sg
    mh = m * (1.0 / (1.0 - B1 ** STEP))
    vh = v * (1.0 / (1.0 - B2 ** STEP))
    w = w_ref[...]
    wn = w - lr * (mh / (jnp.sqrt(vh) + EPS) + DECAY * w)
    wo_ref[...] = wn
    mo_ref[...] = m
    vo_ref[...] = v
    wb_ref[...] = wn.astype(BF16)


def adam(c, g, w, m, v, lr):
    n = w.shape[0]
    bl = 2048
    spec = pl.BlockSpec((bl, 128), lambda i: (i, 0))
    sds = jax.ShapeDtypeStruct((n, 128), F32)
    return pl.pallas_call(
        functools.partial(adam_kernel, lr),
        grid=(n // bl,),
        in_specs=[pl.BlockSpec(memory_space=pltpu.SMEM)] + [spec] * 4,
        out_specs=[spec] * 4,
        out_shape=[sds, sds, sds, jax.ShapeDtypeStruct((n, 128), BF16)],
        compiler_params=pltpu.CompilerParams(dimension_semantics=('arbitrary',), vmem_limit_bytes=48 * 2**20),
        name='adam',
    )(c, g, w, m, v)


def solution(mesh):
    stages = mesh.shape['stage']
    swap = [(0, 1), (1, 0)]

    def device_step(x_in, targets, w_work, w_master, m_prior, v_prior, clip_tau):
        micro, rows, d = x_in.shape
        f = 4 * d
        tokens = micro * rows * 2
        stage = lax.axis_index('stage')
        core0 = lax.axis_index('data') == 0
        half = lax.optimization_barrier(w_master.reshape(-1, 128))
        mine = lax.cond(
            core0,
            lambda w: w.reshape(d, 4, d).astype(BF16).transpose(1, 0, 2).reshape(f, d),
            lambda w: w.reshape(f, d).astype(BF16),
            half)
        stack = lax.all_gather(mine, ('stage', 'data'), axis=0, tiled=True)

        h = lax.dynamic_index_in_dim(x_in, stage, 0, keepdims=False)
        t = lax.dynamic_index_in_dim(targets, stage, 0, keepdims=False)
        xs, us, acts = [], [], []
        for l in range(stages):
            xs.append(h)
            u, a = up(h, stack, 2 * l)
            h = down(a, stack, 2 * l + 1, h)
            us.append(u)
            acts.append(a)
        res = h.astype(F32) - t.astype(F32)
        loss = 0.5 * jnp.sum(res * res)
        g = (res / tokens).astype(BF16)

        parts = [None] * stages

        def dw1(o, c=None):
            m = dot(o[0], o[1], ((0,), (0,)))
            return to_tiles(m if c is None else m + from_tiles(c, d, f))

        def dw2(o, c=None):
            m = dot(o[2], o[3], ((0,), (0,)))
            return to_tiles(m if c is None else m + from_tiles(c, f, d))

        tie = lax.optimization_barrier
        for l in reversed(range(stages)):
            du = du_of(g, stack, 2 * l + 1, us[l])
            ops = (xs[l], du, acts[l], g)
            sent = lax.cond(core0, dw2, dw1, ops)
            came = lax.ppermute(sent, 'data', swap)
            if l > 0:
                g = dx(du, stack, 2 * l, g)
                came, g = tie((came, g))
            own = lax.cond(core0, dw1, dw2, ops, came)
            parts[l] = lax.psum_scatter(own, 'stage', scatter_dimension=0, tiled=True)
        sq = sum(jnp.sum(p * p) for p in parts)
        sums = lax.psum(jnp.stack([sq, loss]), ('stage', 'data'))
        gt = lax.all_to_all(jnp.stack(parts), 'stage', 0, 0)
        gt = gt.reshape(-1, 8, 128)
        grad = lax.cond(
            core0,
            lambda q: from_tiles(q, d, f).reshape(-1, 128),
            lambda q: from_tiles(q, f, d).reshape(-1, 128),
            gt)
        c = jnp.minimum(1.0, clip_tau / jnp.sqrt(sums[0]))
        w_new, m_new, v_new, wb = adam(c.reshape(1), grad, half, m_prior.reshape(-1, 128), v_prior.reshape(-1, 128), LR_BASE / math.sqrt(d))
        wb = lax.all_gather(wb.reshape(1, 1, -1), 'data', axis=2, tiled=True)
        shape = w_master.shape
        return sums[1] / tokens, wb, w_new.reshape(shape), m_new.reshape(shape), v_new.reshape(shape)

    row = P(None, 'data', None)
    shard = P('stage', None, 'data')
    whole = P('stage', None, None)
    return jax.shard_map(device_step, mesh=mesh, in_specs=(row, row, whole, shard, shard, shard, P()), out_specs=(P(), whole, shard, shard, shard), check_vma=False)
```
